128 devices in a mesh: head: 16 (over z, y), batch: 8 (over x, core).
Axes of the slice: x: 4, y: 4, z: 4, core: 2. Of those that a mesh axis runs over, the one named last changes fastest.
Arguments:
- incoming_hidden_stream: bfloat16 [1024, 4096], P('batch'), may hold values from -6 to 6
- reception_projection: bfloat16 [4096, 4096], P(None, 'head'), may hold values from -0.09375 to 0.09375
- address_projection: bfloat16 [4096, 4096], P(None, 'head'), may hold values from -0.09375 to 0.09375
- payload_projection: bfloat16 [4096, 4096], P(None, 'head'), may hold values from -0.09375 to 0.09375
- sigmoid_filter_matrix: bfloat16 [4096, 4096], P(None, 'head'), may hold values from -0.09375 to 0.09375
- forgetting_speed: float32 [1024, 4096], P('batch', 'head'), may hold values from 0.01 to 1.5
- adaptation_step_size: float32 [1024, 4096], P('batch', 'head'), may hold values from 0 to 1
- diagonal_boost: float32 [4096], P('head'), may hold values from -0.6 to 0.6
- subspace_standardize_scale: float32 [4096], P('head'), may hold values from 0.5 to 2
- recurrent_memory_matrix: float32 [128, 64, 64, 64], P('batch', 'head'), may hold values from -6 to 6
- emission_projection: bfloat16 [4096, 4096], P('head'), may hold values from -0.09375 to 0.09375
- closing_standardize_scale: float32 [4096], replicated, may hold values from 0.7 to 2
- lexicon_projection: bfloat16 [4096, 65536], P(None, ('head', 'batch')), may hold values from -32 to 32
- proposed_tokens_list: int32 [128, 8], P('batch'), may hold values from 0 to 65535
- threshold_milli_nats: int32 [128, 8], P('batch'), may hold values from -22000 to -10001
Outputs:
- new_state: float32 [128, 64, 64, 64], P('batch', 'head')
- margin: float32 [128, 8], P('batch')
- accept: float32 [128, 8], P('batch')
The draws below stay inside these ranges and needn't reach their ends.
All inputs are finite; a program needn't handle non-finite values.
Results may differ from the reference program's by a relative error of at most 0.0017.
Values may be sent and summed in bfloat16 or wider, within the bound.
A program may use at most 128 MiB of HBM per device.

```python
import math
import jax
import jax.numpy as jnp
from jax import lax

EMBED_DIM = 4096
ATTN_LANES = 64
SUBSPACE_SIZE = 64
VOCAB = 65536
DRAFT = 8
SEQS = 128
TOKENS = 1024


def draw_closing_standardize_scale(key, part):
    return jax.random.uniform(key, (EMBED_DIM,), jnp.float32, 0.7, 1.4)


def draw_lexicon_projection(key, part):
    noise_key = jax.random.fold_in(key, 11)
    sign_key = jax.random.fold_in(key, 23)
    noise = jnp.clip(jax.random.normal(noise_key, (EMBED_DIM, VOCAB), jnp.float32) * 0.046875, -0.3, 0.3)
    signs = jax.random.randint(sign_key, (EMBED_DIM, 1), 0, 2).astype(jnp.float32) * 2.0 - 1.0
    rowpos = jax.lax.broadcasted_iota(jnp.int32, (EMBED_DIM, 1), 0)
    shifted = jnp.where(rowpos < 8, 32.0 * signs, noise)
    return shifted.astype(jnp.bfloat16)


def place_ends(entries, key, low, top_value):
    longest = entries.shape.index(max(entries.shape))
    spots = []
    for shift in (0, 1):
        where = [jax.random.randint(jax.random.fold_in(key, axis), (), 0, length) for axis, length in enumerate(entries.shape)]
        where[longest] = (where[longest] + shift) % entries.shape[longest]
        spots.append(tuple(where))
    return entries.at[spots[0]].set(low).at[spots[1]].set(top_value)


def levels(stream_key, shape, cuts, smallest, top_value):
    gain = 1.0
    for dim, shards_of in cuts:
        heights = jax.random.uniform(jax.random.fold_in(jax.random.fold_in(stream_key, 6), dim), (shards_of,), jnp.float32, smallest / len(cuts), top_value / len(cuts))
        gain = gain * jnp.repeat(jnp.exp(heights), shape[dim] // shards_of).reshape((-1,) + (1,) * (len(shape) - 1 - dim))
    return gain


def normal_values(rng, dims, scale, bound, shards=(), dtype=jnp.bfloat16):
    drawn = scale * jax.random.normal(rng, dims, jnp.float32)
    if shards:
        drawn = drawn * levels(rng, dims, shards, -0.22, 0.18)
    return jnp.clip(drawn, -bound, bound).astype(dtype)


def setup_inputs(seed: int = 0) -> dict:
    arg_keys = jax.random.split(jax.random.key(seed), 16)
    incoming_hidden_stream = normal_values(arg_keys[0], (TOKENS, EMBED_DIM), 1.0, 6.0, ((0, 8),))
    reception_projection = normal_values(arg_keys[1], (EMBED_DIM, EMBED_DIM), EMBED_DIM ** -0.5, 0.09375, ((1, 16),))
    address_projection = normal_values(arg_keys[2], (EMBED_DIM, EMBED_DIM), EMBED_DIM ** -0.5, 0.09375, ((1, 16),))
    payload_projection = normal_values(arg_keys[3], (EMBED_DIM, EMBED_DIM), EMBED_DIM ** -0.5, 0.09375, ((1, 16),))
    sigmoid_filter_matrix = normal_values(arg_keys[4], (EMBED_DIM, EMBED_DIM), EMBED_DIM ** -0.5, 0.09375, ((1, 16),))
    forgetting_speed = jnp.clip(jnp.exp(math.log(1.5) - 5.0106353 * jax.random.uniform(arg_keys[5], (TOKENS, EMBED_DIM), jnp.float32) ** levels(arg_keys[5], (TOKENS, EMBED_DIM), ((0, 8), (1, 16)), -0.2, 0.2)), 0.01, 1.5)
    adaptation_step_size = jnp.clip(1.0 * jax.random.uniform(arg_keys[6], (TOKENS, EMBED_DIM), jnp.float32) ** levels(arg_keys[6], (TOKENS, EMBED_DIM), ((0, 8), (1, 16)), -0.2, 0.2), 0.0, 1.0)
    diagonal_boost = normal_values(arg_keys[7], (EMBED_DIM,), 0.1, 0.6, ((0, 16),), jnp.float32)
    subspace_standardize_scale = jnp.clip(0.5 + 1.5 * jax.random.uniform(arg_keys[8], (EMBED_DIM,), jnp.float32) ** levels(arg_keys[8], (EMBED_DIM,), ((0, 16),), -0.2, 0.2), 0.5, 2.0)
    recurrent_memory_matrix = normal_values(arg_keys[9], (SEQS, ATTN_LANES, SUBSPACE_SIZE, SUBSPACE_SIZE), 1.0, 6.0, ((0, 8), (1, 16)), jnp.float32)
    emission_projection = normal_values(arg_keys[10], (EMBED_DIM, EMBED_DIM), EMBED_DIM ** -0.5, 0.09375, ((0, 16),))
    closing_standardize_scale = draw_closing_standardize_scale(jax.random.fold_in(arg_keys[15], 71), 0)
    lexicon_projection = draw_lexicon_projection(jax.random.fold_in(arg_keys[15], 71), 0)
    proposed_tokens_list = place_ends(jax.random.randint(arg_keys[13], (SEQS, DRAFT), 0, VOCAB), jax.random.fold_in(arg_keys[13], 1), 0, VOCAB - 1).astype(jnp.int32)
    threshold_milli_nats = place_ends(jax.random.randint(arg_keys[14], (SEQS, DRAFT), -22000, -10000), jax.random.fold_in(arg_keys[14], 1), -22000, (-10000) - 1).astype(jnp.int32)
    return {"incoming_hidden_stream": incoming_hidden_stream, "reception_projection": reception_projection, "address_projection": address_projection, "payload_projection": payload_projection, "sigmoid_filter_matrix": sigmoid_filter_matrix, "forgetting_speed": forgetting_speed, "adaptation_step_size": adaptation_step_size, "diagonal_boost": diagonal_boost, "subspace_standardize_scale": subspace_standardize_scale, "recurrent_memory_matrix": recurrent_memory_matrix, "emission_projection": emission_projection, "closing_standardize_scale": closing_standardize_scale, "lexicon_projection": lexicon_projection, "proposed_tokens_list": proposed_tokens_list, "threshold_milli_nats": threshold_milli_nats}


def advance(start, reception_vectors, address_vectors, payload_vectors, decay, rate):
    unit = address_vectors * lax.rsqrt(lax.optimization_barrier(jnp.mean(address_vectors * address_vectors, -1, keepdims=True)) + 1e-06) / math.sqrt(address_vectors.shape[-1])
    inputs = tuple((jnp.moveaxis(item, 1, 0) for item in (reception_vectors, address_vectors, payload_vectors, decay, unit, rate)))

    def step(current, pieces):
        recept_now, keys_now, values_now, decay_now, unit_now, rate_now = pieces
        recall = jnp.einsum('bhij,bhj->bhi', current, unit_now, precision=lax.Precision.HIGHEST)
        current = current * decay_now[:, :, None, :] - recall[:, :, :, None] * (unit_now * rate_now)[:, :, None, :] + values_now[:, :, :, None] * keys_now[:, :, None, :]
        output = jnp.einsum('bhij,bhj->bhi', current, recept_now, precision=lax.Precision.HIGHEST)
        return (current, output)
    final, outputs = lax.scan(step, start, inputs)
    return (final, jnp.moveaxis(outputs, 0, 1))

def reference(incoming_hidden_stream, reception_projection, address_projection, payload_projection, sigmoid_filter_matrix, forgetting_speed, adaptation_step_size, diagonal_boost, subspace_standardize_scale, recurrent_memory_matrix, emission_projection, closing_standardize_scale, lexicon_projection, proposed_tokens_list, threshold_milli_nats):
    shape4 = (SEQS, DRAFT, ATTN_LANES, SUBSPACE_SIZE)
    reception_vectors = jnp.dot(incoming_hidden_stream, reception_projection, preferred_element_type=jnp.float32).reshape(shape4)
    address_vectors = jnp.dot(incoming_hidden_stream, address_projection, preferred_element_type=jnp.float32).reshape(shape4)
    payload_vectors = jnp.dot(incoming_hidden_stream, payload_projection, preferred_element_type=jnp.float32).reshape(shape4)
    gate = jnp.dot(incoming_hidden_stream, sigmoid_filter_matrix, preferred_element_type=jnp.float32)
    decay = jnp.exp(-forgetting_speed).reshape(shape4)
    rate = adaptation_step_size.reshape(shape4)
    new_state, wkv = advance(recurrent_memory_matrix, reception_vectors, address_vectors, payload_vectors, decay, rate)
    center = wkv - lax.optimization_barrier(jnp.mean(wkv, -1, keepdims=True))
    interpolated_embedding = center * lax.rsqrt(lax.optimization_barrier(jnp.mean(center * center, -1, keepdims=True)) + 1e-05) * subspace_standardize_scale.reshape(ATTN_LANES, SUBSPACE_SIZE)
    interpolated_embedding = interpolated_embedding + lax.optimization_barrier(jnp.sum(reception_vectors * address_vectors * diagonal_boost.reshape(ATTN_LANES, SUBSPACE_SIZE), -1, keepdims=True)) * payload_vectors
    gated = (interpolated_embedding.reshape(TOKENS, EMBED_DIM) * jax.nn.sigmoid(gate)).astype(jnp.bfloat16)
    residual = incoming_hidden_stream.astype(jnp.float32) + jnp.dot(gated, emission_projection, preferred_element_type=jnp.float32)
    centered = residual - lax.optimization_barrier(jnp.mean(residual, -1, keepdims=True))
    normed = (centered * lax.rsqrt(lax.optimization_barrier(jnp.mean(centered * centered, -1, keepdims=True)) + 1e-05) * closing_standardize_scale).astype(jnp.bfloat16)
    logits = jnp.dot(normed, lexicon_projection, preferred_element_type=jnp.float32)
    peak = lax.optimization_barrier(jnp.max(logits, -1))
    total = lax.optimization_barrier(jnp.sum(jnp.exp(logits - peak[:, None]), -1))
    target = jnp.take_along_axis(logits, proposed_tokens_list.reshape(TOKENS, 1).astype(jnp.int32), 1)[:, 0]
    logprob = target - (peak + jnp.log(total))
    margin = logprob.reshape(SEQS, DRAFT) - threshold_milli_nats.astype(jnp.float32) / 1000.0
    accept = jnp.cumprod(jax.nn.sigmoid(margin * 0.5), axis=1)
    return (new_state, margin, accept)
```

```python
import math

import jax
import jax.numpy as jnp
from jax import lax
from jax.experimental import pallas as pl
from jax.experimental.pallas import tpu as pltpu
from jax.sharding import Mesh
from jax.sharding import PartitionSpec as P

HEAD = ("head_0", "head_1")
HEAD_BATCH = ("head_0", "head_1", "batch")


def in_blocks(x, dim, size):
    before, after = (x.shape[:dim], x.shape[dim + 1 :])
    return jnp.moveaxis(x.reshape(*before, size, -1, *after), dim, 0)


def sent_and_summed(x, axis, dim):
    size = lax.axis_size(axis)
    parts = lax.all_to_all(in_blocks(x, dim, size), axis, 0, 0, tiled=True)
    return jnp.sum(parts, axis=0)


def by_axis(x, axes):
    for axis in axes:
        x = lax.psum(x, axis)
    return x


def joined_along(parts, dim):
    parts = jnp.moveaxis(parts, 0, dim)
    shape = parts.shape
    return parts.reshape(*shape[:dim], shape[dim] * shape[dim + 1], *shape[dim + 2 :])


def sent_to_all(x, axis):
    copies = jnp.broadcast_to(x, (lax.axis_size(axis), *x.shape))
    return lax.all_to_all(copies, axis, split_axis=0, concat_axis=0, tiled=True)


def gathered_copies(x, axis, dim):
    return joined_along(sent_to_all(x, axis), dim)


def gathered_once(x, axis):
    leaves = jax.tree.leaves(x)
    sequence = sorted(range(len(leaves)), key=lambda k: -leaves[k].size)
    width = (1, *leaves[sequence[0]].shape)[-1]
    lines = [
        jnp.pad(leaves[k].reshape(-1), (0, -leaves[k].size % width)).reshape(-1, width)
        for k in sequence
    ]
    both, at, found = (sent_to_all(jnp.concatenate(lines), axis), 0, {})
    for k, line in zip(sequence, lines):
        share = both[:, at : at + len(line)].reshape(len(both), -1)
        found[k] = share[:, : leaves[k].size].reshape(-1, *leaves[k].shape)
        at += len(line)
    numbers = iter(range(len(leaves)))
    return jax.tree.map(lambda _: found[next(numbers)], x)


def combined_pairwise(pieces, combine):
    while len(jax.tree.leaves(pieces)[0]) > 1:
        pieces = jax.vmap(combine)(
            *(jax.tree.map(lambda part: part[side::2], pieces) for side in (0, 1))
        )
    return jax.tree.map(lambda part: part[0], pieces)


def combined_all(x, axis, combine):
    pieces = gathered_once(x, axis)
    return combined_pairwise(pieces, combine)


def gathered_by_type(x, axis):
    leaves, found = (jax.tree.leaves(x), {})
    for initial, a in enumerate(leaves):
        if initial not in found:
            alike = [k for k, b in enumerate(leaves) if b.dtype == a.dtype]
            got = (
                gathered_once([leaves[k] for k in alike], axis)
                if len(alike) > 1
                else [sent_to_all(a, axis)]
            )
            for k, b in zip(alike, got):
                found[k] = b
    numbers = iter(range(len(leaves)))
    return jax.tree.map(lambda _: found[next(numbers)], x)


def merged(x, axis, combine):
    pieces = gathered_by_type(x, axis)
    return combined_pairwise(pieces, combine)


def halves(x):
    high = x.astype(jnp.bfloat16)
    return high, (x - high.astype(jnp.float32)).astype(jnp.bfloat16)


def rows_dot(a, b):
    rows = a.shape[1]
    a_high, a_low = halves(a)
    b_high, b_low = halves(b)
    dims = (((2,), (2,)), ((0,), (0,)))
    both = lax.dot_general(
        jnp.concatenate([a_high, a_low], 1), b_high, dims, preferred_element_type=jnp.float32
    )
    rest = lax.dot_general(a_high, b_low, dims, preferred_element_type=jnp.float32)
    return both[:, :rows] + both[:, rows:] + rest


def outer_dot(a, b):
    a_high, a_low = halves(a)
    b_high, b_low = halves(b)
    return lax.dot_general(
        jnp.concatenate([a_high, a_high, a_low], 1),
        jnp.concatenate([b_high, b_low, b_high], 1),
        (((1,), (1,)), ((0,), (0,))),
        preferred_element_type=jnp.float32,
    )


def summed_speeds(speeds):
    place = lax.broadcasted_iota(jnp.int32, speeds.shape, 1)
    for shift in (1, 2, 4):
        speeds = speeds + jnp.where(place >= shift, pltpu.roll(speeds, shift, 1), 0.0)
    return speeds


def mix_kernel(
    x_ref, wr_ref, wk_ref, wv_ref, wg_ref, speed_ref, rate_ref, boost_ref, scale_ref, state_ref,
    new_ref, gated_ref, acc,
):
    step = pl.program_id(0)

    @pl.when(step == 0)
    def _():
        acc[...] = jnp.zeros_like(acc)

    x = x_ref[...]
    for n, w_ref in enumerate((wr_ref, wk_ref, wv_ref, wg_ref)):
        acc[n] += jnp.dot(x, w_ref[...], preferred_element_type=jnp.float32)

    @pl.when(step == pl.num_programs(0) - 1)
    def _():
        seqs, lanes, size, _ = state_ref.shape
        shape = (seqs, -1, size)
        line = lax.broadcasted_iota(jnp.int32, (1, 16, 16), 1)
        source = lax.broadcasted_iota(jnp.int32, (1, 16, 16), 2) % 8
        seen = source < jnp.where(line < 8, line, line - 7)
        for h in range(lanes):
            cut = slice(h * size, (h + 1) * size)
            recept, keys, values, gate = (acc[n, :, cut].reshape(shape) for n in range(4))
            speed = speed_ref[:, cut].reshape(shape)
            spent = summed_speeds(speed)
            last = spent[:, 7:8, :]
            unit = keys * lax.rsqrt(jnp.mean(keys * keys, -1, keepdims=True) + 1e-06) / math.sqrt(size)
            eased = unit * rate_ref[:, cut].reshape(shape)
            grown = jnp.exp(spent)
            asks = jnp.concatenate([unit * jnp.exp(speed - spent), recept * jnp.exp(-spent)], 1)
            gains = jnp.concatenate([keys * grown, eased * grown], 1)
            weights = jnp.where(seen, rows_dot(asks, gains), 0.0)
            start = state_ref[:, h]
            found = rows_dot(asks, start)
            for t in range(8):
                found = found + weights[:, :, t : t + 1] * values[:, t : t + 1, :]
            for t in range(8):
                found = found - weights[:, :, 8 + t : 9 + t] * found[:, t : t + 1, :]
            recall, wkv = found[:, :8], found[:, 8:]
            left = jnp.exp(spent - last)
            new_ref[:, h] = start * jnp.exp(-last) + outer_dot(
                jnp.concatenate([values, -recall], 1),
                jnp.concatenate([keys * left, eased * left], 1),
            )
            center = wkv - jnp.mean(wkv, -1, keepdims=True)
            mixed = (
                center
                * lax.rsqrt(jnp.mean(center * center, -1, keepdims=True) + 1e-05)
                * scale_ref[:, cut].reshape(1, 1, size)
            )
            own = jnp.sum(recept * keys * boost_ref[:, cut].reshape(1, 1, size), -1, keepdims=True)
            mixed = mixed + own * values
            gated = mixed * jax.nn.sigmoid(gate)
            gated_ref[:, cut] = gated.reshape(-1, size).astype(gated_ref.dtype)


def mixed_tokens(x, wr, wk, wv, wg, speed, rate, boost, scale, state):
    tokens, width = x.shape
    columns = wr.shape[1]
    depth = 512
    whole = lambda *shape: pl.BlockSpec(shape, lambda k: (0,) * len(shape))
    piece = pl.BlockSpec((depth, columns), lambda k: (k, 0))
    return pl.pallas_call(
        mix_kernel,
        grid=(width // depth,),
        in_specs=[pl.BlockSpec((tokens, depth), lambda k: (0, k)), piece, piece, piece, piece]
        + [whole(tokens, columns)] * 2
        + [whole(1, columns)] * 2
        + [whole(*state.shape)],
        out_specs=[whole(*state.shape), whole(tokens, columns)],
        out_shape=[
            jax.ShapeDtypeStruct(state.shape, jnp.float32),
            jax.ShapeDtypeStruct((tokens, columns), jnp.bfloat16),
        ],
        scratch_shapes=[pltpu.VMEM((4, tokens, columns), jnp.float32)],
        compiler_params=pltpu.CompilerParams(vmem_limit_bytes=40 * 1024 * 1024),
        name="mix",
    )(x, wr, wk, wv, wg, speed, rate, boost.reshape(1, -1), scale.reshape(1, -1), state)


def combine_stats(first, second):
    top = jnp.maximum(first[0], second[0])
    summed = first[1] * jnp.exp(first[0] - top) + second[1] * jnp.exp(second[0] - top)
    return (top, summed, first[2] + second[2])


def local_stats(logits, ids_flat, offset):
    peak = jnp.max(logits, -1)
    total = jnp.sum(jnp.exp(logits - peak[:, None]), -1)
    column = lax.broadcasted_iota(jnp.int32, logits.shape, 1)
    target = jnp.sum(jnp.where(column == (ids_flat - offset)[:, None], logits, 0.0), -1)
    return (peak, total, target)


def shards(
    incoming_hidden_stream,
    reception_projection,
    address_projection,
    payload_projection,
    sigmoid_filter_matrix,
    forgetting_speed,
    adaptation_step_size,
    diagonal_boost,
    subspace_standardize_scale,
    recurrent_memory_matrix,
    emission_projection,
    closing_standardize_scale,
    lexicon_projection,
    proposed_tokens_list,
    threshold_milli_nats,
):
    seq_dev, draft_len = proposed_tokens_list.shape
    tok_dev = seq_dev * draft_len
    width = incoming_hidden_stream.shape[1]
    new_state, gated = mixed_tokens(
        incoming_hidden_stream,
        reception_projection,
        address_projection,
        payload_projection,
        sigmoid_filter_matrix,
        forgetting_speed,
        adaptation_step_size,
        diagonal_boost,
        subspace_standardize_scale,
        recurrent_memory_matrix,
    )
    partial_out = jnp.dot(gated, emission_projection, preferred_element_type=jnp.float32)
    share = sent_and_summed(partial_out, HEAD, 1)
    cols = share.shape[1]
    begin = lax.axis_index(HEAD) * cols
    residual = (
        lax.dynamic_slice_in_dim(incoming_hidden_stream, begin, cols, 1).astype(jnp.float32) + share
    )
    moment_one, moment_two = (
        by_axis(jnp.sum(residual, -1), HEAD),
        by_axis(jnp.sum(residual * residual, -1), HEAD),
    )
    mean_row = moment_one / width
    variance = moment_two / width - mean_row * mean_row
    gain_part = lax.dynamic_slice_in_dim(closing_standardize_scale, begin, cols, 0)
    normed_part = (
        (residual - mean_row[:, None]) * lax.rsqrt(variance + 1e-05)[:, None] * gain_part
    ).astype(jnp.bfloat16)
    normed = gathered_copies(normed_part, HEAD, 1)
    every, every_ids = (
        lax.all_gather(normed, "batch", axis=0, tiled=True),
        lax.all_gather(proposed_tokens_list, "batch", axis=0, tiled=True),
    )
    logits = jnp.dot(every, lexicon_projection, preferred_element_type=jnp.float32)
    vcols = lexicon_projection.shape[1]
    offset = (lax.axis_index(HEAD) * lax.axis_size("batch") + lax.axis_index("batch")) * vcols
    peak, total, target = local_stats(logits, every_ids.reshape(-1), offset)
    peak, total, target = combined_all((peak, total, target), "batch", combine_stats)
    row_begin = lax.axis_index("batch") * tok_dev
    peak = lax.dynamic_slice_in_dim(peak, row_begin, tok_dev, 0)
    total = lax.dynamic_slice_in_dim(total, row_begin, tok_dev, 0)
    target = lax.dynamic_slice_in_dim(target, row_begin, tok_dev, 0)
    top, summed, target = merged((peak, total, target), HEAD, combine_stats)
    logprob = target - (top + jnp.log(summed))
    margin = logprob.reshape(seq_dev, draft_len) - threshold_milli_nats.astype(jnp.float32) / 1000.0
    accept = jnp.cumprod(jax.nn.sigmoid(margin * 0.5), axis=1)
    return (new_state, margin, accept)


def solution(mesh):
    split = Mesh(mesh.devices.reshape(4, 4, mesh.shape["batch"]), ("head_0", "head_1", "batch"))
    return jax.shard_map(
        shards,
        mesh=split,
        in_specs=(
            P("batch", None),
            P(None, HEAD),
            P(None, HEAD),
            P(None, HEAD),
            P(None, HEAD),
            P("batch", HEAD),
            P("batch", HEAD),
            P(HEAD),
            P(HEAD),
            P("batch", HEAD, None, None),
            P(HEAD, None),
            P(),
            P(None, HEAD_BATCH),
            P("batch", None),
            P("batch", None),
        ),
        out_specs=(P("batch", HEAD, None, None), P("batch", None), P("batch", None)),
        check_vma=False,
    )
```
